256 devices in a mesh: row: 64 (over z_hi, x, y, core), rep: 4 (over z_lo).
Axes of the slice: x: 4, y: 4, z: 8 (z_hi: 2, z_lo: 4; z = z_hi * 4 + z_lo), core: 2. Of those that a mesh axis runs over, the one named last changes fastest.
Arguments:
- features: bfloat16 [32768, 128], P('row'), may hold values from -6 to 6
- tiles: bfloat16 [4096, 4, 256, 256], P('row', 'rep'), may hold values from -0.375 to 0.375
- tile_where: int32 [4096, 4, 2], P('row', 'rep'), may hold values from 0 to 127, as said below
- tile_count: int32 [64, 4], P('row', 'rep'), may hold values from 1 to 64, as said below
- degree: int32 [32768], P('row'), may hold values from 1 to 8
- self_one: bfloat16 [128, 256], replicated, may hold values from -0.5 to 0.5
- neigh_one: bfloat16 [128, 256], replicated, may hold values from -0.5 to 0.5
- self_two: bfloat16 [256, 256], replicated, may hold values from -0.375 to 0.375
- neigh_two: bfloat16 [256, 256], replicated, may hold values from -0.375 to 0.375
Outputs:
- embedding: float32 [32768, 256], P('row')
The draws below stay inside these ranges and needn't reach their ends.
Inputs may be any that keep to these rules, and one draw needn't show every extreme that they name: `tile_where`: column 0 is a tile row of 0 to 1, column 1 a tile column of 0 to 127. `tile_count`: some block row and replica has all 64 slots live in every draw.
All inputs are finite; a program needn't handle non-finite values.
Results may differ from the reference program's by a relative error of at most 0.005.
Values may be sent and summed in bfloat16 or wider, within the bound.
No kernel may reach another device: no remote copies, remote signals or barrier semaphores. Data moves between devices by JAX's collectives and lax.ppermute only.
A program may use at most 128 MiB of HBM per device.

```python
import jax
import jax.numpy as jnp
from jax import lax

FIN = 128
HID = 256
TILE = 256
ROWS_DEV = 512
SLOTS = 64
NODES = 32768
N_ROW = 64
N_REP = 4


def draw_tile_where(key, part):
    total_rows = NODES // ROWS_DEV * SLOTS
    key_rows = jax.random.fold_in(key, 11)
    key_cols = jax.random.fold_in(key, 12)
    tile_rows = jax.random.randint(key_rows, (total_rows, N_REP, 1), 0, ROWS_DEV // TILE, dtype=jnp.int32)
    tile_cols = jax.random.randint(key_cols, (total_rows, N_REP, 1), 0, NODES // TILE, dtype=jnp.int32)
    return jnp.concatenate([tile_rows, tile_cols], axis=2)


def draw_tile_count(key, part):
    blocks = NODES // ROWS_DEV
    key_base = jax.random.fold_in(key, 21)
    key_heavy = jax.random.fold_in(key, 22)
    key_full = jax.random.fold_in(key, 23)
    base = jax.random.randint(key_base, (blocks, N_REP), max(1, SLOTS // 2), SLOTS + 1, dtype=jnp.int32)
    heavy = jax.random.randint(key_heavy, (blocks, N_REP), 0, 8, dtype=jnp.int32) == 0
    counts = jnp.where(heavy, SLOTS, base)
    chosen = jax.random.randint(key_full, (), 0, blocks * N_REP, dtype=jnp.int32)
    places = jnp.arange(blocks * N_REP, dtype=jnp.int32).reshape(blocks, N_REP)
    return jnp.where(places == chosen, SLOTS, counts).astype(jnp.int32)


def with_ends(entries, rng, least, high):
    dims = entries.shape
    place = [jax.random.randint(jax.random.fold_in(rng, axis), (), 0, dims[axis]) for axis in range(len(dims))]
    entries = entries.at[tuple(place)].set(least)
    longest = dims.index(max(dims))
    place[longest] = (place[longest] + 1) % dims[longest]
    return entries.at[tuple(place)].set(high)


def levels(own_key, shape, shards, least, high):
    level, own = 1.0, jax.random.fold_in(own_key, 6)
    for axis_at, blocks in shards:
        steps = jnp.exp(jax.random.uniform(jax.random.fold_in(own, axis_at), (blocks,), jnp.float32, least / len(shards), high / len(shards)))
        level = level * jnp.repeat(steps, shape[axis_at] // blocks).reshape([-1 if axis == axis_at else 1 for axis in range(len(shape))])
    return level


def centred(key, dims, spread, reach, pieces=(), held_as=jnp.bfloat16):
    gain = levels(key, dims, pieces, -0.22, 0.18) if pieces else 1.0
    drawn = jax.random.normal(key, dims, jnp.float32) * spread * gain
    return jnp.minimum(jnp.maximum(drawn, -reach), reach).astype(held_as)


def setup_inputs(seed: int = 0) -> dict:
    streams_of = jax.random.split(jax.random.key(seed), 10)
    features = centred(streams_of[0], (NODES, FIN), 1.0, 6.0, ((0, 64),))
    tiles = centred(streams_of[1], (N_ROW * SLOTS, N_REP, TILE, TILE), TILE ** -0.5, 0.375, ((0, 64), (1, 4)))
    tile_where = draw_tile_where(jax.random.fold_in(streams_of[9], 71), 0)
    tile_count = draw_tile_count(jax.random.fold_in(streams_of[9], 71), 0)
    degree = with_ends(jax.random.randint(streams_of[4], (NODES,), 1, 9), jax.random.fold_in(streams_of[4], 1), 1, 8).astype(jnp.int32)
    self_one = centred(streams_of[5], (FIN, HID), FIN ** -0.5, 0.5)
    neigh_one = centred(streams_of[6], (FIN, HID), FIN ** -0.5, 0.5)
    self_two = centred(streams_of[7], (HID, HID), HID ** -0.5, 0.375)
    neigh_two = centred(streams_of[8], (HID, HID), HID ** -0.5, 0.375)
    return dict(features=features, tiles=tiles, tile_where=tile_where, tile_count=tile_count, degree=degree, self_one=self_one, neigh_one=neigh_one, self_two=self_two, neigh_two=neigh_two)


def adjacency_product(values, tiles, tile_where, tile_count):
    width = values.shape[1]
    per_block = ROWS_DEV // TILE
    blocks = values.reshape(-1, TILE, width)
    tiles_all = tiles.reshape(N_ROW, SLOTS, N_REP, TILE, TILE)
    where_all = tile_where.reshape(N_ROW, SLOTS, N_REP, 2)

    def one_row(operands):
        tile_block, where_block, count_block = operands
        columns = jnp.take(blocks, where_block[..., 1], axis=0)
        products = jnp.einsum('scij,scjf->scif', tile_block.astype(jnp.float32), columns.astype(jnp.float32), precision=lax.Precision.HIGHEST)
        live = jnp.arange(SLOTS, dtype=jnp.int32)[:, None] < count_block[None, :]
        placing = (where_block[..., 0][..., None] == jnp.arange(per_block, dtype=jnp.int32)) & live[..., None]
        summed = jnp.einsum('sct,scif->tif', placing.astype(jnp.float32), products, precision=lax.Precision.HIGHEST)
        return summed.reshape(ROWS_DEV, width)

    partial_value = lax.map(one_row, (tiles_all, where_all, tile_count))
    return partial_value.reshape(-1, width)


def reference(features, tiles, tile_where, tile_count, degree, self_one, neigh_one, self_two, neigh_two):
    scale = degree.astype(jnp.float32)[:, None]
    agg_one = (adjacency_product(features, tiles, tile_where, tile_count) / scale).astype(jnp.bfloat16)
    first = jnp.dot(features, self_one, preferred_element_type=jnp.float32) + jnp.dot(agg_one, neigh_one, preferred_element_type=jnp.float32)
    hidden = jax.nn.relu(first).astype(jnp.bfloat16)
    agg_two = (adjacency_product(hidden, tiles, tile_where, tile_count) / scale).astype(jnp.bfloat16)
    return jnp.dot(hidden, self_two, preferred_element_type=jnp.float32) + jnp.dot(agg_two, neigh_two, preferred_element_type=jnp.float32)
```

```python
import jax
import jax.numpy as jnp
from jax import lax
from jax.experimental import pallas as pl
from jax.experimental.pallas import tpu as pltpu
from jax.sharding import Mesh
from jax.sharding import PartitionSpec as P

TILE = 256
SLOTS = 64
UNROLL = 4
PIECES = 16
PIECE_ROWS = 2048
MIB = 1 << 20


ROW = ("zh", "x", "y", "c")
ORDER = (1, 3, 2)
SWAP = [(0, 1), (1, 0)]


def shift(size, k):
    return [(i, (i + k) % size) for i in range(size)]


def spread(first, second):
    line_a, line_b = [first], [second]
    for k in ORDER:
        line_a.append(lax.ppermute(first, "x", shift(4, k)))
        line_b.append(lax.ppermute(second, "y", shift(4, k)))
    line_a, line_b = jnp.concatenate(line_a), jnp.concatenate(line_b)
    plane_a, plane_b = [line_a], [line_b]
    for k in ORDER:
        plane_a.append(lax.ppermute(line_a, "y", shift(4, k)))
        plane_b.append(lax.ppermute(line_b, "x", shift(4, k)))
    mine = plane_a + plane_b
    return mine + [lax.ppermute(piece, "c", SWAP) for piece in mine]


def place_of(distance):
    return jnp.where(distance == 3, 2, jnp.where(distance == 2, 3, distance))


def slot_places(column):
    half = column % 2
    block = column // 2
    core, y, x, zh = block % 2, (block // 2) % 4, (block // 8) % 4, block // 32
    dx = place_of((lax.axis_index("x") - x) % 4)
    dy = place_of((lax.axis_index("y") - y) % 4)
    dc = core ^ lax.axis_index("c")
    outer = jnp.where(half == 0, dy, dx)
    inner = jnp.where(half == 0, dx, dy)
    return ((dc * 2 + half) * 4 + outer) * 8 + inner * 2 + zh


def gather_pieces(pieces, whole):
    for p, piece in enumerate(pieces):

        def move(j, carry, p=p, piece=piece):
            source = pl.ds(pl.multiple_of(j * TILE, TILE), TILE)
            target = pl.ds(pl.multiple_of(p * PIECE_ROWS + j * TILE, TILE), TILE)
            whole[target, :] = piece[source, :]
            return carry

        lax.fori_loop(0, PIECE_ROWS // TILE, move, 0)


def tile_rows(index):
    return pl.ds(pl.multiple_of(index * TILE, TILE), TILE)


def write_quarters(me, total, outs):
    for k, out in enumerate(outs):
        start = pl.multiple_of(((me + k) % 4) * 128, 128)
        out[...] = total[pl.ds(start, 128), :].astype(out.dtype)


def first_kernel(place, segment, scalars, tiles, *refs):
    pieces, refs = refs[:PIECES], refs[PIECES:]
    quarters, chosen, whole, total = refs[:4], refs[4], refs[5], refs[6]
    gather_pieces(pieces, whole)
    total[...] = jnp.zeros_like(total)

    def step(g, carry):
        for u in range(UNROLL):
            s = g * UNROLL + u
            block = whole[tile_rows(place[s]), :]
            chosen[tile_rows(s), :] = block
            product = jnp.dot(tiles[s], block, preferred_element_type=jnp.float32)
            total[tile_rows(segment[s]), :] += product
        return carry

    lax.fori_loop(0, scalars[0], step, 0)
    write_quarters(scalars[1], total, quarters)


def second_kernel(place, segment, scalars, tiles, chosen, weights, *refs):
    pieces, refs = refs[:PIECES], refs[PIECES:]
    quarters, whole, total = refs[:4], refs[4], refs[5]
    gather_pieces(pieces, whole)
    total[...] = jnp.zeros_like(total)

    def step(g, carry):
        for u in range(UNROLL):
            s = g * UNROLL + u
            both = jnp.concatenate([chosen[tile_rows(s), :], whole[tile_rows(place[s]), :]], axis=1)
            hidden = jnp.dot(both, weights[...], preferred_element_type=jnp.float32)
            hidden = jnp.maximum(hidden, 0.0).astype(jnp.bfloat16)
            product = jnp.dot(tiles[s], hidden, preferred_element_type=jnp.float32)
            total[tile_rows(segment[s]), :] += product
        return carry

    lax.fori_loop(0, scalars[0], step, 0)
    write_quarters(scalars[1], total, quarters)


def last_kernel(scalars, own, weights, *refs):
    shares, out = refs[:4], refs[4]
    for k, share in enumerate(shares):
        start = pl.multiple_of(((scalars[1] + 4 - k) % 4) * 128, 128)
        rows = pl.ds(start, 128)
        out[rows, :] = own[rows, :] + jnp.dot(
            share[...], weights[...], preferred_element_type=jnp.float32
        )


def in_vmem():
    return pl.BlockSpec(memory_space=pltpu.VMEM)


def in_smem():
    return pl.BlockSpec(memory_space=pltpu.SMEM)


def quarter_shapes(width):
    return [
        jax.ShapeDtypeStruct((128, width), jnp.float32 if k == 0 else jnp.bfloat16)
        for k in range(4)
    ]


def reduced(quarters, scale):
    total = quarters[0]
    for k in (1, 3, 2):
        total = total + lax.ppermute(quarters[k], "zl", shift(4, k)).astype(jnp.float32)
    return (total / scale).astype(jnp.bfloat16)


def per_device(
    features, tiles, tile_where, tile_count, degree, self_one, neigh_one, self_two, neigh_two
):
    zh, zl = lax.axis_index("zh"), lax.axis_index("zl")
    tile_block = tiles.reshape(SLOTS, TILE, TILE)
    where_block = tile_where.reshape(SLOTS, 2)
    count = tile_count.reshape(())
    live = jnp.arange(SLOTS, dtype=jnp.int32) < count
    segment = jnp.where(live, where_block[:, 0], 2)
    place = jnp.where(live, slot_places(where_block[:, 1]), 0).astype(jnp.int32)
    scalars = jnp.stack([(count + UNROLL - 1) // UNROLL, zl]).astype(jnp.int32)
    scale = lax.dynamic_slice_in_dim(degree, zl * 128, 128, 0).astype(jnp.float32)[:, None]

    other = lax.ppermute(features, "zh", SWAP)
    low = jnp.where(zh == 0, features, other)
    high = jnp.where(zh == 0, other, features)
    first = jnp.concatenate([low[:TILE], high[:TILE]])
    second = jnp.concatenate([low[TILE:], high[TILE:]])
    pieces = spread(first, second)
    *quarters, chosen = pl.pallas_call(
        first_kernel,
        out_shape=quarter_shapes(128)
        + [jax.ShapeDtypeStruct((SLOTS * TILE, 128), jnp.bfloat16)],
        in_specs=[in_smem()] * 3 + [in_vmem()] * (1 + PIECES),
        out_specs=[in_vmem()] * 5,
        scratch_shapes=[
            pltpu.VMEM((PIECES * PIECE_ROWS, 128), jnp.bfloat16),
            pltpu.VMEM((3 * TILE, 128), jnp.float32),
        ],
    )(place, segment, scalars, tile_block, *pieces)

    agg_one = reduced(quarters, scale)
    column = lax.all_to_all(
        jnp.broadcast_to(agg_one[None], (8, 128, 128)), ("zh", "zl"), 0, 0, tiled=True
    )
    first = jnp.concatenate([column[0:2], column[4:6]]).reshape(2 * TILE, 128)
    second = jnp.concatenate([column[2:4], column[6:8]]).reshape(2 * TILE, 128)
    pieces = spread(first, second)

    own_agg = lax.dynamic_slice_in_dim(column, zh * 4, 4, 0).reshape(2 * TILE, 128)
    weights = jnp.concatenate([self_one, neigh_one])
    own_hidden = jnp.dot(
        jnp.concatenate([features, own_agg], axis=1), weights, preferred_element_type=jnp.float32
    )
    own_hidden = jax.nn.relu(own_hidden).astype(jnp.bfloat16)
    own_part = jnp.dot(own_hidden, self_two, preferred_element_type=jnp.float32)

    quarters = pl.pallas_call(
        second_kernel,
        out_shape=quarter_shapes(256),
        in_specs=[in_smem()] * 3 + [in_vmem()] * (3 + PIECES),
        out_specs=[in_vmem()] * 4,
        scratch_shapes=[
            pltpu.VMEM((PIECES * PIECE_ROWS, 128), jnp.bfloat16),
            pltpu.VMEM((3 * TILE, 256), jnp.float32),
        ],
    )(place, segment, scalars, tile_block, chosen, weights, *pieces)

    agg_two = reduced(quarters, scale)
    shares = [agg_two] + [lax.ppermute(agg_two, "zl", shift(4, k)) for k in (1, 2, 3)]
    return pl.pallas_call(
        last_kernel,
        out_shape=jax.ShapeDtypeStruct((512, 256), jnp.float32),
        in_specs=[in_smem()] + [in_vmem()] * 6,
        out_specs=in_vmem(),
    )(scalars, own_part, neigh_two, *shares)


def solution(mesh):
    wide = Mesh(mesh.devices.reshape(2, 4, 4, 2, 4), ("zh", "x", "y", "c", "zl"))
    return jax.shard_map(
        per_device,
        mesh=wide,
        in_specs=(
            P(ROW, None),
            P(ROW, "zl", None, None),
            P(ROW, "zl", None),
            P(ROW, "zl"),
            P(ROW),
            P(),
            P(),
            P(),
            P(),
        ),
        out_specs=P(ROW, None),
        check_vma=False,
    )
```

```python
import jax
import jax.numpy as jnp
from jax import lax
from jax.experimental import pallas as pl
from jax.experimental.pallas import tpu as pltpu
from jax.sharding import Mesh
from jax.sharding import PartitionSpec as P

TILE = 256
SLOTS = 64
UNROLL = 4
LISTED = SLOTS + UNROLL
PIECE_ROWS = 4096
EARLY = 6
LATE = 2
MIB = 1 << 20


ROW = ("zh", "x", "y", "c")
ORDER = (1, 3, 2)
SWAP = [(0, 1), (1, 0)]


def shift(size, k):
    return [(i, (i + k) % size) for i in range(size)]


def spread(first, second):
    line_a, line_b = [first], [second]
    for k in ORDER:
        line_a.append(lax.ppermute(first, "x", shift(4, k)))
        line_b.append(lax.ppermute(second, "y", shift(4, k)))
    line_a, line_b = jnp.concatenate(line_a), jnp.concatenate(line_b)
    plane_a, plane_b = [line_a], [line_b]
    for k in ORDER:
        plane_a.append(lax.ppermute(line_a, "y", shift(4, k)))
        plane_b.append(lax.ppermute(line_b, "x", shift(4, k)))
    pairs = [jnp.concatenate(pair) for pair in zip(plane_a, plane_b)]
    early = pairs[:3] + [lax.ppermute(pair, "c", SWAP) for pair in pairs[:3]]
    return early, [pairs[3], lax.ppermute(pairs[3], "c", SWAP)]


def plan_kernel(where, count, early, late, groups):
    my_x, my_y, my_core = lax.axis_index("x"), lax.axis_index("y"), lax.axis_index("c")

    def step(s, carry):
        n_early, n_late = carry
        segment, column = where[2 * s], where[2 * s + 1]
        half = column & 1
        core = ((column >> 1) & 1) ^ my_core
        dy = (my_y - (column >> 2)) & 3
        dx = (my_x - (column >> 4)) & 3
        dy = dy ^ (dy >> 1)
        dx = dx ^ (dx >> 1)
        outer = jnp.where(half == 0, dy, dx)
        inner = jnp.where(half == 0, dx, dy)
        is_late = (outer == 3).astype(jnp.int32)
        piece = jnp.where(outer == 3, core, core * 3 + outer)
        place = piece * 16 + half * 8 + inner * 2 + (column >> 6)
        code = s + segment * 256 + place * 65536
        early[n_early] = code
        late[n_late] = code
        return n_early + 1 - is_late, n_late + is_late

    n_early, n_late = lax.fori_loop(0, count[0], step, (0, 0))
    for u in range(UNROLL):
        early[n_early + u] = 2 * 256
        late[n_late + u] = 2 * 256
    groups[0] = (n_early + UNROLL - 1) >> 2
    groups[1] = (n_late + UNROLL - 1) >> 2


def gather_pieces(pieces, whole):
    for p, piece in enumerate(pieces):

        def move(j, carry, p=p, piece=piece):
            source = pl.ds(pl.multiple_of(j * TILE, TILE), TILE)
            target = pl.ds(pl.multiple_of(p * PIECE_ROWS + j * TILE, TILE), TILE)
            whole[target, :] = piece[source, :]
            return carry

        lax.fori_loop(0, PIECE_ROWS // TILE, move, 0)


def tile_rows(index):
    return pl.ds(pl.multiple_of(index * TILE, TILE), TILE)


def write_quarters(total, outs):
    me = lax.axis_index("zl")
    for k, out in enumerate(outs):
        start = pl.multiple_of(((me + k) & 3) * 128, 128)
        out[...] = total[pl.ds(start, 128), :].astype(out.dtype)


def each(groups, body):
    def step(g, carry):
        for u in range(UNROLL):
            body(g * UNROLL + u)
        return carry

    lax.fori_loop(0, groups, step, 0)


def first_layer(listed, groups, tiles, pieces, chosen, whole, total, held, tile_sem, out_sem):
    def tile_copy(at):
        return pltpu.make_async_copy(tiles.at[listed[at] & 255], held.at[at], tile_sem.at[at])

    def chosen_copy(at):
        rows = whole.at[tile_rows(listed[at] >> 16), :]
        return pltpu.make_async_copy(rows, chosen.at[tile_rows(at), :], out_sem.at[at])

    def multiply(at):
        code = listed[at]
        chosen_copy(at).start()
        tile_copy(at).wait()
        block = whole[tile_rows(code >> 16), :]
        product = jnp.dot(held[at], block, preferred_element_type=jnp.float32)
        total[tile_rows((code >> 8) & 255), :] += product

    each(groups, lambda at: tile_copy(at).start())
    gather_pieces(pieces, whole)
    each(groups, multiply)
    each(groups, lambda at: chosen_copy(at).wait())


def second_layer(
    listed, groups, tiles, chosen, weights, pieces, whole, total, held, kept, tile_sem, kept_sem
):
    def tile_copy(at):
        return pltpu.make_async_copy(tiles.at[listed[at] & 255], held.at[at], tile_sem.at[at])

    def kept_copy(at):
        rows = tile_rows(at)
        return pltpu.make_async_copy(chosen.at[rows, :], kept.at[rows, :], kept_sem.at[at])

    def fetch(at):
        kept_copy(at).start()
        tile_copy(at).start()

    def multiply(at):
        code = listed[at]
        kept_copy(at).wait()
        both = jnp.concatenate([kept[tile_rows(at), :], whole[tile_rows(code >> 16), :]], axis=1)
        hidden = jnp.dot(both, weights[...], preferred_element_type=jnp.float32)
        hidden = jnp.maximum(hidden, 0.0).astype(jnp.bfloat16)
        tile_copy(at).wait()
        product = jnp.dot(held[at], hidden, preferred_element_type=jnp.float32)
        total[tile_rows((code >> 8) & 255), :] += product

    each(groups, fetch)
    gather_pieces(pieces, whole)
    each(groups, multiply)


def first_early(listed, groups, tiles, *refs):
    pieces, (total, chosen, whole, *rest) = refs[:EARLY], refs[EARLY:]
    total[...] = jnp.zeros_like(total)
    first_layer(listed, groups[0], tiles, pieces, chosen, whole, total, *rest)


def first_late(listed, groups, tiles, before, *refs):
    pieces, refs = refs[:LATE], refs[LATE:]
    quarters, (chosen, whole, total, *rest) = refs[:4], refs[4:]
    total[...] = before[...]
    first_layer(listed, groups[1], tiles, pieces, chosen, whole, total, *rest)
    write_quarters(total, quarters)


def second_early(listed, groups, tiles, chosen, weights, *refs):
    pieces, (total, whole, *rest) = refs[:EARLY], refs[EARLY:]
    total[...] = jnp.zeros_like(total)
    second_layer(listed, groups[0], tiles, chosen, weights, pieces, whole, total, *rest)


def second_late(listed, groups, tiles, chosen, weights, before, *refs):
    pieces, refs = refs[:LATE], refs[LATE:]
    quarters, (whole, total, *rest) = refs[:4], refs[4:]
    total[...] = before[...]
    second_layer(listed, groups[1], tiles, chosen, weights, pieces, whole, total, *rest)
    write_quarters(total, quarters)


def last_kernel(own, weights, *refs):
    shares, out = refs[:4], refs[4]
    me = lax.axis_index("zl")
    for k, share in enumerate(shares):
        rows = pl.ds(pl.multiple_of(((me - k) & 3) * 128, 128), 128)
        out[rows, :] = own[rows, :] + jnp.dot(
            share[...], weights[...], preferred_element_type=jnp.float32
        )


def in_vmem():
    return pl.BlockSpec(memory_space=pltpu.VMEM)


def in_smem():
    return pl.BlockSpec(memory_space=pltpu.SMEM)


def in_hbm():
    return pl.BlockSpec(memory_space=pltpu.HBM)


def call(kernel, smem, hbm, vmem, outs, spaces, scratch=(), limit=4, flops=1):
    return pl.pallas_call(
        kernel,
        out_shape=outs,
        in_specs=[in_smem()] * len(smem) + [in_hbm()] * len(hbm) + [in_vmem()] * len(vmem),
        out_specs=[pl.BlockSpec(memory_space=space) for space in spaces],
        scratch_shapes=list(scratch),
        compiler_params=pltpu.CompilerParams(vmem_limit_bytes=limit * MIB),
        cost_estimate=pl.CostEstimate(flops=flops, transcendentals=0, bytes_accessed=1 << 20),
    )(*smem, *hbm, *vmem)


def quarter_shapes(width, sent):
    return [
        jax.ShapeDtypeStruct((128, width), jnp.float32 if k == 0 else sent) for k in range(4)
    ]


def reduced(quarters, scale):
    total = quarters[0]
    for k in ORDER:
        total = total + lax.ppermute(quarters[k], "zl", shift(4, k)).astype(jnp.float32)
    return (total / scale).astype(jnp.bfloat16)


def per_device(
    features, tiles, tile_where, tile_count, degree, self_one, neigh_one, self_two, neigh_two
):
    zh, zl = lax.axis_index("zh"), lax.axis_index("zl")
    tile_block = pltpu.with_memory_space_constraint(
        tiles.reshape(SLOTS, TILE, TILE), pltpu.HBM
    )
    ints = jax.ShapeDtypeStruct((LISTED,), jnp.int32)
    early_list, late_list, groups = call(
        plan_kernel,
        (tile_where.reshape(2 * SLOTS), tile_count.reshape(1)),
        (),
        (),
        [ints, ints, jax.ShapeDtypeStruct((2,), jnp.int32)],
        [pltpu.SMEM] * 3,
    )
    scale = lax.dynamic_slice_in_dim(degree, zl * 128, 128, 0).astype(jnp.float32)[:, None]
    weights = jnp.concatenate([self_one, neigh_one])

    other = lax.ppermute(features, "zh", SWAP)
    low = jnp.where(zh == 0, features, other)
    high = jnp.where(zh == 0, other, features)
    first = jnp.concatenate([low[:TILE], high[:TILE]])
    second = jnp.concatenate([low[TILE:], high[TILE:]])
    first, second, early_list, late_list, groups, scale, weights = lax.optimization_barrier(
        (first, second, early_list, late_list, groups, scale, weights)
    )
    chosen_shape = pltpu.HBM((LISTED * TILE, 128), jnp.bfloat16)
    early_whole = pltpu.VMEM((EARLY * PIECE_ROWS, 128), jnp.bfloat16)
    late_whole = pltpu.VMEM((LATE * PIECE_ROWS, 128), jnp.bfloat16)
    held = pltpu.VMEM((LISTED, TILE, TILE), jnp.bfloat16)
    kept = pltpu.VMEM((LISTED * TILE, 128), jnp.bfloat16)
    sems = [pltpu.SemaphoreType.DMA((LISTED,))] * 2

    early, late = spread(first, second)
    total, early_chosen = call(
        first_early,
        (early_list, groups),
        (tile_block,),
        early,
        [jax.ShapeDtypeStruct((3 * TILE, 128), jnp.float32), chosen_shape],
        [pltpu.VMEM, pltpu.HBM],
        [early_whole, held, *sems],
        18,
        1 << 31,
    )
    *quarters, late_chosen = call(
        first_late,
        (late_list, groups),
        (tile_block,),
        (total, *late),
        quarter_shapes(128, jnp.float32) + [chosen_shape],
        [pltpu.VMEM] * 4 + [pltpu.HBM],
        [late_whole, pltpu.VMEM((3 * TILE, 128), jnp.float32), held, *sems],
        15,
        1 << 29,
    )

    agg_one = reduced(quarters, scale)
    column = lax.all_to_all(
        jnp.broadcast_to(agg_one[None], (8, 128, 128)), ("zh", "zl"), 0, 0, tiled=True
    )
    first = jnp.concatenate([column[0:2], column[4:6]]).reshape(2 * TILE, 128)
    second = jnp.concatenate([column[2:4], column[6:8]]).reshape(2 * TILE, 128)

    own_agg = lax.dynamic_slice_in_dim(column, zh * 4, 4, 0).reshape(2 * TILE, 128)
    own_hidden = jnp.dot(
        jnp.concatenate([features, own_agg], axis=1), weights, preferred_element_type=jnp.float32
    )
    own_hidden = jax.nn.relu(own_hidden).astype(jnp.bfloat16)
    own_part = jnp.dot(own_hidden, self_two, preferred_element_type=jnp.float32)

    early, late = spread(first, second)
    (total,) = call(
        second_early,
        (early_list, groups),
        (tile_block, early_chosen),
        (weights, *early),
        [jax.ShapeDtypeStruct((3 * TILE, 256), jnp.float32)],
        [pltpu.VMEM],
        [early_whole, held, kept, *sems],
        24,
        1 << 32,
    )
    quarters = call(
        second_late,
        (late_list, groups),
        (tile_block, late_chosen),
        (weights, total, *late),
        quarter_shapes(256, jnp.bfloat16),
        [pltpu.VMEM] * 4,
        [late_whole, pltpu.VMEM((3 * TILE, 256), jnp.float32), held, kept, *sems],
        20,
        1 << 30,
    )

    agg_two = reduced(quarters, scale)
    shares = [agg_two] + [lax.ppermute(agg_two, "zl", shift(4, k)) for k in (1, 2, 3)]
    (out,) = call(
        last_kernel,
        (),
        (),
        (own_part, neigh_two, *shares),
        [jax.ShapeDtypeStruct((512, 256), jnp.float32)],
        [pltpu.VMEM],
    )
    return out


def solution(mesh):
    wide = Mesh(mesh.devices.reshape(2, 4, 4, 2, 4), ("zh", "x", "y", "c", "zl"))
    return jax.shard_map(
        per_device,
        mesh=wide,
        in_specs=(
            P(ROW, None),
            P(ROW, "zl", None, None),
            P(ROW, "zl", None),
            P(ROW, "zl"),
            P(ROW),
            P(),
            P(),
            P(),
            P(),
        ),
        out_specs=P(ROW, None),
        check_vma=False,
    )
```

```python
import jax
import jax.numpy as jnp
from jax import lax
from jax.experimental import pallas as pl
from jax.experimental.pallas import tpu as pltpu
from jax.sharding import Mesh
from jax.sharding import PartitionSpec as P

TILE = 256
SLOTS = 64
UNROLL = 4
NODES = 32768
MIB = 1 << 20


ROW = ("zh", "x", "y", "c")
PLANE = ("x", "y", "c")
ORDER = (1, 3, 2)
SWAP = [(0, 1), (1, 0)]


def shift(size, k):
    return [(i, (i + k) % size) for i in range(size)]


def in_plane(k, phase):
    pairs = []
    for x in range(4):
        for y in range(4):
            for c in range(2):
                along_x = (c + phase) % 2 == 0
                to_x, to_y = ((x + k) % 4, y) if along_x else (x, (y + k) % 4)
                pairs.append(((x * 4 + y) * 2 + c, (to_x * 4 + to_y) * 2 + c))
    return pairs


def hops(value, phase):
    return [lax.ppermute(value, PLANE, in_plane(k, phase)) for k in ORDER]


def spread(block, *extras):
    other = lax.ppermute(block, "zh", SWAP)
    other, *extras = lax.optimization_barrier((other, *extras))
    line = jnp.concatenate([block, *hops(block, 0)])
    own = jnp.concatenate([line, *hops(line, 1)])
    line = jnp.concatenate([other, *hops(other, 0)])
    one, three, two = hops(line, 1)
    near = jnp.concatenate([line, one, three])
    own_swapped = lax.ppermute(own, "c", SWAP)
    near_swapped = lax.ppermute(near, "c", SWAP)
    two_swapped = lax.ppermute(two, "c", SWAP)
    return [own, near, two, own_swapped, near_swapped, two_swapped], *extras


def plan_kernel(where, count, tiles, listed, groups, held, sem):
    load = pltpu.make_async_copy(tiles, held, sem)
    load.start()
    my_zh, my_core = lax.axis_index("zh"), lax.axis_index("c")
    my_x, my_y = lax.axis_index("x"), lax.axis_index("y")

    def step(s, carry):
        segment, column = where[0, s], where[1, s]
        core = (column >> 1) & 1
        dy = (my_y - (column >> 2)) & 3
        dx = (my_x - (column >> 4)) & 3
        dy = dy ^ (dy >> 1)
        dx = dx ^ (dx >> 1)
        outer = jnp.where(core == 0, dy, dx)
        inner = jnp.where(core == 0, dx, dy)
        part = (core ^ my_core) * 2 + ((column >> 6) ^ my_zh)
        place = part * 32 + outer * 8 + inner * 2 + (column & 1)
        segment = jnp.where(s < count[0, 0], segment, 2)
        listed[s] = segment + place * 256
        return carry

    lax.fori_loop(0, SLOTS, step, 0)
    groups[0] = (count[0, 0] + UNROLL - 1) >> 2
    load.wait()


def gather_pieces(pieces, whole):
    base = 0
    for piece in pieces:

        def move(j, carry, base=base, piece=piece):
            source = pl.ds(pl.multiple_of(j * TILE, TILE), TILE)
            target = pl.ds(pl.multiple_of(base + j * TILE, TILE), TILE)
            whole[target, :] = piece[source, :]
            return carry

        lax.fori_loop(0, piece.shape[0] // TILE, move, 0)
        base += piece.shape[0]


def tile_rows(index):
    return pl.ds(pl.multiple_of(index * TILE, TILE), TILE)


def write_quarters(total, outs):
    me = lax.axis_index("zl")
    for k, out in enumerate(outs):
        start = pl.multiple_of(((me + k) & 3) * 128, 128)
        out[...] = total[pl.ds(start, 128), :].astype(out.dtype)


def first_kernel(listed, groups, tiles, *refs):
    pieces, quarters, (whole, total) = refs[:6], refs[6:10], refs[10:]
    gather_pieces(pieces, whole)
    total[...] = jnp.zeros_like(total)

    def step(g, carry):
        products = []
        for u in range(UNROLL):
            block = whole[tile_rows(listed[g * UNROLL + u] >> 8), :]
            tile = tiles[g * UNROLL + u]
            products.append(jnp.dot(tile, block, preferred_element_type=jnp.float32))
        for u in range(UNROLL):
            total[tile_rows(listed[g * UNROLL + u] & 255), :] += products[u]
        return carry

    lax.fori_loop(0, groups[0], step, 0)
    write_quarters(total, quarters)


def second_kernel(listed, groups, tiles, features, weights, *refs):
    pieces, quarters, (whole, total) = refs[:6], refs[6:10], refs[10:]
    gather_pieces(pieces, whole)
    total[...] = jnp.zeros_like(total)

    def step(g, carry):
        for u in range(UNROLL):
            rows = tile_rows(listed[g * UNROLL + u] >> 8)
            both = jnp.concatenate([features[rows, :], whole[rows, :]], axis=1)
            hidden = jnp.dot(both, weights[...], preferred_element_type=jnp.float32)
            hidden = jnp.maximum(hidden, 0.0).astype(jnp.bfloat16)
            tile = tiles[g * UNROLL + u]
            product = jnp.dot(tile, hidden, preferred_element_type=jnp.float32)
            total[tile_rows(listed[g * UNROLL + u] & 255), :] += product
        return carry

    lax.fori_loop(0, groups[0], step, 0)
    write_quarters(total, quarters)


def arrange_kernel(*refs):
    shares, out = refs[:4], refs[4]
    me = lax.axis_index("zl")
    for k, share in enumerate(shares):
        out[pl.ds(pl.multiple_of(((me - k) & 3) * 128, 128), 128), :] = share[...]


def last_kernel(own, weights, *refs):
    shares, out = refs[:4], refs[4]
    me = lax.axis_index("zl")
    for k, share in enumerate(shares):
        rows = pl.ds(pl.multiple_of(((me - k) & 3) * 128, 128), 128)
        out[rows, :] = own[rows, :] + jnp.dot(
            share[...], weights[...], preferred_element_type=jnp.float32
        )


def space(kind):
    return pl.BlockSpec(memory_space=kind)


def call(kernel, smem, hbm, vmem, outs, kinds, scratch=(), limit=4, flops=1 << 20):
    return pl.pallas_call(
        kernel,
        out_shape=outs,
        in_specs=[space(pltpu.SMEM)] * len(smem)
        + [space(pltpu.HBM)] * len(hbm)
        + [space(pltpu.VMEM)] * len(vmem),
        out_specs=[space(kind) for kind in kinds],
        scratch_shapes=list(scratch),
        compiler_params=pltpu.CompilerParams(vmem_limit_bytes=limit * MIB),
        cost_estimate=pl.CostEstimate(flops=flops, transcendentals=0, bytes_accessed=1 << 20),
    )(*smem, *hbm, *vmem)


def quarter_shapes(width, sent):
    return [
        jax.ShapeDtypeStruct((128, width), jnp.float32 if k == 0 else sent) for k in range(4)
    ]


def over_rep(values):
    return {k: lax.ppermute(values[k], "zl", shift(4, k)) for k in ORDER}


def reduced(quarters, scale):
    total = quarters[0]
    for piece in over_rep(quarters).values():
        total = total + piece.astype(jnp.float32)
    return (total / scale).astype(jnp.bfloat16)


def shared(value):
    got = over_rep([value] * 4)
    return [value, got[1], got[2], got[3]]


def per_device(
    features, tiles, tile_where, tile_count, degree, self_one, neigh_one, self_two, neigh_two
):
    zl = lax.axis_index("zl")
    listed, groups, tiles_held = call(
        plan_kernel,
        (tile_where.reshape(SLOTS, 2).T, tile_count),
        (
            pltpu.with_memory_space_constraint(
                tiles.reshape(SLOTS, TILE, TILE), pltpu.HBM
            ),
        ),
        (),
        [
            jax.ShapeDtypeStruct((SLOTS,), jnp.int32),
            jax.ShapeDtypeStruct((1,), jnp.int32),
            pltpu.VMEM((SLOTS, TILE, TILE), jnp.bfloat16),
        ],
        [pltpu.SMEM, pltpu.SMEM, pltpu.VMEM],
        [pltpu.SemaphoreType.DMA],
        2,
    )
    scale = lax.dynamic_slice_in_dim(degree, zl * 128, 128, 0).astype(jnp.float32)[:, None]
    weights = jnp.concatenate([self_one, neigh_one])
    whole = pltpu.VMEM((NODES, 128), jnp.bfloat16)

    pieces, scale, weights = spread(features, scale, weights)
    *quarters, features_held = call(
        first_kernel,
        (listed, groups),
        (),
        (tiles_held, *pieces),
        quarter_shapes(128, jnp.float32) + [whole],
        [pltpu.VMEM] * 5,
        [pltpu.VMEM((3 * TILE, 128), jnp.float32)],
        8,
        1 << 30,
    )

    agg_one = reduced(quarters, scale)
    (own_agg,) = call(
        arrange_kernel,
        (),
        (),
        shared(agg_one),
        [jax.ShapeDtypeStruct((512, 128), jnp.bfloat16)],
        [pltpu.VMEM],
    )
    own_hidden = jnp.dot(
        jnp.concatenate([features, own_agg], axis=1), weights, preferred_element_type=jnp.float32
    )
    own_hidden = jax.nn.relu(own_hidden).astype(jnp.bfloat16)
    own_part = jnp.dot(own_hidden, self_two, preferred_element_type=jnp.float32)

    (pieces,) = spread(own_agg)
    quarters = call(
        second_kernel,
        (listed, groups),
        (),
        (tiles_held, features_held, weights, *pieces),
        quarter_shapes(256, jnp.bfloat16),
        [pltpu.VMEM] * 4,
        [whole, pltpu.VMEM((3 * TILE, 256), jnp.float32)],
        14,
        1 << 31,
    )

    (out,) = call(
        last_kernel,
        (),
        (),
        (own_part, neigh_two, *shared(reduced(quarters, scale))),
        [jax.ShapeDtypeStruct((512, 256), jnp.float32)],
        [pltpu.VMEM],
    )
    return out


def solution(mesh):
    wide = Mesh(mesh.devices.reshape(2, 4, 4, 2, 4), ("zh", "x", "y", "c", "zl"))
    return jax.shard_map(
        per_device,
        mesh=wide,
        in_specs=(
            P(ROW, None),
            P(ROW, "zl", None, None),
            P(ROW, "zl", None),
            P(ROW, "zl"),
            P(ROW),
            P(),
            P(),
            P(),
            P(),
        ),
        out_specs=P(ROW, None),
        check_vma=False,
    )
```

```python
import jax
import jax.numpy as jnp
from jax import lax
from jax.experimental import pallas as pl
from jax.experimental.pallas import tpu as pltpu
from jax.sharding import Mesh
from jax.sharding import PartitionSpec as P

TILE = 256
SLOTS = 64
UNROLL = 4
NODES = 32768
MIB = 1 << 20


ROW = ("zh", "x", "y", "c")
PLANE = ("x", "y", "c")
ORDER = (1, 3, 2)
SWAP = [(0, 1), (1, 0)]


def in_plane(k, phase):
    pairs = []
    for x in range(4):
        for y in range(4):
            for c in range(2):
                along_x = (c + phase) % 2 == 0
                to_x, to_y = ((x + k) % 4, y) if along_x else (x, (y + k) % 4)
                pairs.append(((x * 4 + y) * 2 + c, (to_x * 4 + to_y) * 2 + c))
    return pairs


def hops(value, phase, order=ORDER):
    received = []
    for k in order:
        received.append(lax.ppermute(value, PLANE, in_plane(k, phase)))
    return received


def onward(one, three):
    half = one.shape[0] // 2
    top = lax.ppermute(one[:half], PLANE, in_plane(1, 1))
    bottom = lax.ppermute(three[half:], PLANE, in_plane(3, 1))
    return jnp.concatenate([top, bottom])


def spread(block):
    other = lax.ppermute(block, "zh", SWAP)
    own_line = jnp.concatenate([block, *hops(block, 0)])
    other_line = jnp.concatenate([other, *hops(other, 0)])
    pieces = []
    for line in (own_line, other_line):
        one, three = hops(line, 1, (1, 3))
        pieces += [jnp.concatenate([line, one, three]), onward(one, three)]
    swapped = []
    for piece in pieces:
        swapped.append(lax.ppermute(piece, "c", SWAP))
    return pieces + swapped


def load_kernel(tiles, held, sem):
    load = pltpu.make_async_copy(tiles, held, sem)
    load.start()
    load.wait()


def plan_kernel(where, count, degree, self_one, neigh_one, listed, groups, scale, weights):
    my_zh, my_core = lax.axis_index("zh"), lax.axis_index("c")
    my_x, my_y = lax.axis_index("x"), lax.axis_index("y")

    def step(s, carry):
        segment, column = where[0, s], where[1, s]
        core = (column >> 1) & 1
        dy = (my_y - (column >> 2)) & 3
        dx = (my_x - (column >> 4)) & 3
        dy = dy ^ (dy >> 1)
        dx = dx ^ (dx >> 1)
        outer = jnp.where(core == 0, dy, dx)
        inner = jnp.where(core == 0, dx, dy)
        part = (core ^ my_core) * 2 + ((column >> 6) ^ my_zh)
        place = part * 32 + outer * 8 + inner * 2 + (column & 1)
        segment = jnp.where(s < count[0, 0], segment, 2)
        listed[s] = segment + place * 256
        return carry

    lax.fori_loop(0, SLOTS, step, 0)
    groups[0] = (count[0, 0] + UNROLL - 1) >> 2
    share = degree[pl.ds(lax.axis_index("zl"), 1), :].astype(jnp.float32)
    scale[...] = jnp.broadcast_to(share, (128, 128)).T
    weights[pl.ds(0, 128), :] = self_one[...]
    weights[pl.ds(128, 128), :] = neigh_one[...]


def gather_pieces(pieces, whole):
    base = 0
    for piece in pieces:

        def move(j, carry, base=base, piece=piece):
            source = pl.ds(pl.multiple_of(j * TILE, TILE), TILE)
            target = pl.ds(pl.multiple_of(base + j * TILE, TILE), TILE)
            whole[target, :] = piece[source, :]
            return carry

        lax.fori_loop(0, piece.shape[0] // TILE, move, 0)
        base += piece.shape[0]


def tile_rows(index):
    return pl.ds(pl.multiple_of(index * TILE, TILE), TILE)


def write_quarters(total, outs):
    me = lax.axis_index("zl")
    for k, out in enumerate(outs):
        start = pl.multiple_of((me ^ k) * 128, 128)
        out[...] = total[pl.ds(start, 128), :].astype(out.dtype)


def first_kernel(listed, groups, tiles, *refs):
    pieces, quarters, (whole, total) = refs[:8], refs[8:12], refs[12:]
    gather_pieces(pieces, whole)
    total[...] = jnp.zeros_like(total)

    def step(g, carry):
        products = []
        for u in range(UNROLL):
            block = whole[tile_rows(listed[g * UNROLL + u] >> 8), :]
            tile = tiles[g * UNROLL + u]
            products.append(jnp.dot(tile, block, preferred_element_type=jnp.float32))
        for u in range(UNROLL):
            total[tile_rows(listed[g * UNROLL + u] & 255), :] += products[u]
        return carry

    lax.fori_loop(0, groups[0], step, 0)
    write_quarters(total, quarters)


def second_kernel(listed, groups, tiles, features, weights, *refs):
    pieces, quarters, (whole, total) = refs[:8], refs[8:12], refs[12:]
    gather_pieces(pieces, whole)
    total[...] = jnp.zeros_like(total)

    def step(g, carry):
        for u in range(UNROLL):
            rows = tile_rows(listed[g * UNROLL + u] >> 8)
            both = jnp.concatenate([features[rows, :], whole[rows, :]], axis=1)
            hidden = jnp.dot(both, weights[...], preferred_element_type=jnp.float32)
            hidden = jnp.maximum(hidden, 0.0).astype(jnp.bfloat16)
            tile = tiles[g * UNROLL + u]
            product = jnp.dot(tile, hidden, preferred_element_type=jnp.float32)
            total[tile_rows(listed[g * UNROLL + u] & 255), :] += product
        return carry

    lax.fori_loop(0, groups[0], step, 0)
    write_quarters(total, quarters)


def arrange_kernel(*refs):
    shares, out = refs[:4], refs[4]
    me = lax.axis_index("zl")
    for k, share in enumerate(shares):
        out[pl.ds(pl.multiple_of((me ^ k) * 128, 128), 128), :] = share[...]


def last_kernel(own, weights, *refs):
    shares, out = refs[:4], refs[4]
    me = lax.axis_index("zl")
    for k, share in enumerate(shares):
        rows = pl.ds(pl.multiple_of((me ^ k) * 128, 128), 128)
        out[rows, :] = own[rows, :] + jnp.dot(
            share[...], weights[...], preferred_element_type=jnp.float32
        )


def space(kind):
    return pl.BlockSpec(memory_space=kind)


def call(kernel, smem, hbm, vmem, outs, kinds, scratch=(), limit=4, flops=1 << 20):
    return pl.pallas_call(
        kernel,
        out_shape=outs,
        in_specs=[space(pltpu.SMEM)] * len(smem)
        + [space(pltpu.HBM)] * len(hbm)
        + [space(pltpu.VMEM)] * len(vmem),
        out_specs=[space(kind) for kind in kinds],
        scratch_shapes=list(scratch),
        compiler_params=pltpu.CompilerParams(vmem_limit_bytes=limit * MIB),
        cost_estimate=pl.CostEstimate(flops=flops, transcendentals=0, bytes_accessed=1 << 20),
    )(*smem, *hbm, *vmem)


def quarter_shapes(width, sent):
    return [
        jax.ShapeDtypeStruct((128, width), jnp.float32 if k == 0 else sent) for k in range(4)
    ]


def over_rep(values):
    return {k: lax.ppermute(values[k], "zl", [(i, i ^ k) for i in range(4)]) for k in (1, 2, 3)}


def reduced(quarters, scale):
    total = quarters[0]
    for piece in over_rep(quarters).values():
        total = total + piece.astype(jnp.float32)
    scale = jnp.concatenate([scale] * (total.shape[1] // 128), axis=1)
    return (total / scale).astype(jnp.bfloat16)


def shared(value):
    got = over_rep([value] * 4)
    return [value, got[1], got[2], got[3]]


def per_device(
    features, tiles, tile_where, tile_count, degree, self_one, neigh_one, self_two, neigh_two
):
    listed, groups, scale, weights = call(
        plan_kernel,
        (tile_where.reshape(SLOTS, 2).T, tile_count),
        (),
        (degree.reshape(4, 128), self_one, neigh_one),
        [
            jax.ShapeDtypeStruct((SLOTS,), jnp.int32),
            jax.ShapeDtypeStruct((1,), jnp.int32),
            jax.ShapeDtypeStruct((128, 128), jnp.float32),
            jax.ShapeDtypeStruct((256, 256), jnp.bfloat16),
        ],
        [pltpu.SMEM, pltpu.SMEM, pltpu.VMEM, pltpu.VMEM],
        limit=2,
    )
    (tiles_held,) = call(
        load_kernel,
        (),
        (
            pltpu.with_memory_space_constraint(
                tiles.reshape(SLOTS, TILE, TILE), pltpu.HBM
            ),
        ),
        (),
        [pltpu.VMEM((SLOTS, TILE, TILE), jnp.bfloat16)],
        [pltpu.VMEM],
        [pltpu.SemaphoreType.DMA],
        2,
    )
    whole = pltpu.VMEM((NODES, 128), jnp.bfloat16)

    pieces = spread(features)
    *quarters, features_held = call(
        first_kernel,
        (listed, groups),
        (),
        (tiles_held, *pieces),
        quarter_shapes(128, jnp.float32) + [whole],
        [pltpu.VMEM] * 5,
        [pltpu.VMEM((3 * TILE, 128), jnp.float32)],
        8,
        1 << 30,
    )

    agg_one = reduced(quarters, scale)
    (own_agg,) = call(
        arrange_kernel,
        (),
        (),
        shared(agg_one),
        [jax.ShapeDtypeStruct((512, 128), jnp.bfloat16)],
        [pltpu.VMEM],
    )
    own_hidden = jnp.dot(
        jnp.concatenate([features, own_agg], axis=1), weights, preferred_element_type=jnp.float32
    )
    own_hidden = jax.nn.relu(own_hidden).astype(jnp.bfloat16)
    own_part = jnp.dot(own_hidden, self_two, preferred_element_type=jnp.float32)

    pieces = spread(own_agg)
    quarters = call(
        second_kernel,
        (listed, groups),
        (),
        (tiles_held, features_held, weights, *pieces),
        quarter_shapes(256, jnp.bfloat16),
        [pltpu.VMEM] * 4,
        [whole, pltpu.VMEM((3 * TILE, 256), jnp.float32)],
        14,
        1 << 31,
    )

    (out,) = call(
        last_kernel,
        (),
        (),
        (own_part, neigh_two, *shared(reduced(quarters, scale))),
        [jax.ShapeDtypeStruct((512, 256), jnp.float32)],
        [pltpu.VMEM],
    )
    return out


def solution(mesh):
    wide = Mesh(mesh.devices.reshape(2, 4, 4, 2, 4), ("zh", "x", "y", "c", "zl"))
    return jax.shard_map(
        per_device,
        mesh=wide,
        in_specs=(
            P(ROW, None),
            P(ROW, "zl", None, None),
            P(ROW, "zl", None),
            P(ROW, "zl"),
            P(ROW),
            P(),
            P(),
            P(),
            P(),
        ),
        out_specs=P(ROW, None),
        check_vma=False,
    )
```

```python
import jax
import jax.numpy as jnp
from jax import lax
from jax.experimental import pallas as pl
from jax.experimental.pallas import tpu as pltpu
from jax.sharding import Mesh
from jax.sharding import PartitionSpec as P

TILE = 256
SLOTS = 64
UNROLL = 4
LISTED = SLOTS + UNROLL
NODES = 32768
MIB = 1 << 20


ROW = ("zh", "x", "y", "c")
PLANE = ("x", "y", "c")
ORDER = (1, 3, 2)
SWAP = [(0, 1), (1, 0)]


def in_plane(k, phase):
    pairs = []
    for x in range(4):
        for y in range(4):
            for c in range(2):
                along_x = (c + phase) % 2 == 0
                to_x, to_y = ((x + k) % 4, y) if along_x else (x, (y + k) % 4)
                pairs.append(((x * 4 + y) * 2 + c, (to_x * 4 + to_y) * 2 + c))
    return pairs


def hops(value, phase, order=ORDER):
    received = []
    for k in order:
        received.append(lax.ppermute(value, PLANE, in_plane(k, phase)))
    return received


def onward(one, three):
    half = one.shape[0] // 2
    top = lax.ppermute(one[:half], PLANE, in_plane(1, 1))
    bottom = lax.ppermute(three[half:], PLANE, in_plane(3, 1))
    return jnp.concatenate([top, bottom])


def spread(block):
    other = lax.ppermute(block, "zh", SWAP)
    own_line = jnp.concatenate([block, *hops(block, 0)])
    other_line = jnp.concatenate([other, *hops(other, 0)])
    one, three = hops(own_line, 1, (1, 3))
    own_near, own_two = jnp.concatenate([own_line, one, three]), onward(one, three)
    one, three = hops(other_line, 1, (1, 3))
    middle = jnp.concatenate([other_line, one, three, own_two])
    pieces = [own_near, middle, onward(one, three)]
    swapped = []
    for piece in pieces:
        swapped.append(lax.ppermute(piece, "c", SWAP))
    return pieces + swapped


def load_kernel(tiles, held, sem):
    load = pltpu.make_async_copy(tiles, held, sem)
    load.start()
    load.wait()


def plan_kernel(
    where, count, degree, self_one, neigh_one, early, late, groups, scale, weights
):
    my_zh, my_core = lax.axis_index("zh"), lax.axis_index("c")
    my_x, my_y = lax.axis_index("x"), lax.axis_index("y")

    def step(s, carry):
        n_early, n_late = carry
        segment, column = where[0, s], where[1, s]
        core = (column >> 1) & 1
        dy = (my_y - (column >> 2)) & 3
        dx = (my_x - (column >> 4)) & 3
        dy = dy ^ (dy >> 1)
        dx = dx ^ (dx >> 1)
        outer = jnp.where(core == 0, dy, dx)
        inner = jnp.where(core == 0, dx, dy)
        dz = (column >> 6) ^ my_zh
        part = jnp.where(outer == 3, 48 + dz * 8, dz * 24 + outer * 8)
        place = (core ^ my_core) * 64 + part + inner * 2 + (column & 1)
        code = s + segment * 256 + place * 65536
        early[n_early] = code
        late[n_late] = code
        is_late = jnp.where(outer == 3, 1, dz)
        return n_early + 1 - is_late, n_late + is_late

    n_early, n_late = lax.fori_loop(0, count[0, 0], step, (0, 0))
    for u in range(UNROLL):
        early[n_early + u] = 2 * 256
        late[n_late + u] = 2 * 256
    groups[0] = (n_early + UNROLL - 1) >> 2
    groups[1] = (n_late + UNROLL - 1) >> 2
    share = degree[pl.ds(lax.axis_index("zl"), 1), :].astype(jnp.float32)
    scale[...] = jnp.broadcast_to(share, (128, 128)).T
    weights[pl.ds(0, 128), :] = self_one[...]
    weights[pl.ds(128, 128), :] = neigh_one[...]


def gather_pieces(pieces, whole, base):
    for piece in pieces:

        def move(j, carry, base=base, piece=piece):
            source = pl.ds(pl.multiple_of(j * TILE, TILE), TILE)
            target = pl.ds(pl.multiple_of(base + j * TILE, TILE), TILE)
            whole[target, :] = piece[source, :]
            return carry

        lax.fori_loop(0, piece.shape[0] // TILE, move, 0)
        base += piece.shape[0]


def tile_rows(index):
    return pl.ds(pl.multiple_of(index * TILE, TILE), TILE)


def write_quarters(total, outs):
    me = lax.axis_index("zl")
    for k, out in enumerate(outs):
        start = pl.multiple_of((me ^ k) * 128, 128)
        out[...] = total[pl.ds(start, 128), :].astype(out.dtype)


def add_products(listed, groups, tiles, rows_of, total):
    def step(g, carry):
        codes = [listed[g * UNROLL + u] for u in range(UNROLL)]
        products = [
            jnp.dot(tiles[code & 255], rows_of(code >> 16), preferred_element_type=jnp.float32)
            for code in codes
        ]
        for code, product in zip(codes, products):
            total[tile_rows((code >> 8) & 255), :] += product
        return carry

    lax.fori_loop(0, groups, step, 0)


def hidden_rows(features, weights, agg):
    def rows_of(place):
        both = jnp.concatenate([features[tile_rows(place), :], agg(place)], axis=1)
        hidden = jnp.dot(both, weights[...], preferred_element_type=jnp.float32)
        return jnp.maximum(hidden, 0.0).astype(jnp.bfloat16)

    return rows_of


def first_kernel(early, late, groups, tiles, *refs):
    pieces, quarters, (whole, total) = refs[:6], refs[6:10], refs[10:]
    gather_pieces(pieces, whole, 0)
    total[...] = jnp.zeros_like(total)
    for which, listed in enumerate((early, late)):
        add_products(
            listed, groups[which], tiles, lambda place: whole[tile_rows(place), :], total
        )
    write_quarters(total, quarters)


def second_early(early, groups, tiles, features, weights, own, swapped, total):
    def agg(place):
        rows = tile_rows(place & 63)
        return jnp.where(place >= 64, swapped[rows, :], own[rows, :])

    total[...] = jnp.zeros_like(total)
    add_products(early, groups[0], tiles, hidden_rows(features, weights, agg), total)


def second_late(late, groups, tiles, features, weights, before, *refs):
    pieces, quarters, (whole, total) = refs[:4], refs[4:8], refs[8:]
    gather_pieces(pieces[:2], whole, 6144)
    gather_pieces(pieces[2:], whole, NODES // 2 + 6144)
    total[...] = before[...]
    agg = lambda place: whole[tile_rows(place), :]
    add_products(late, groups[1], tiles, hidden_rows(features, weights, agg), total)
    write_quarters(total, quarters)


def arrange_kernel(*refs):
    shares, out = refs[:4], refs[4]
    me = lax.axis_index("zl")
    for k, share in enumerate(shares):
        out[pl.ds(pl.multiple_of((me ^ k) * 128, 128), 128), :] = share[...]


def last_kernel(own, weights, *refs):
    shares, out = refs[:4], refs[4]
    me = lax.axis_index("zl")
    for k, share in enumerate(shares):
        rows = pl.ds(pl.multiple_of((me ^ k) * 128, 128), 128)
        out[rows, :] = own[rows, :] + jnp.dot(
            share[...], weights[...], preferred_element_type=jnp.float32
        )


def space(kind):
    return pl.BlockSpec(memory_space=kind)


def call(kernel, smem, hbm, vmem, outs, kinds, scratch=(), limit=4, flops=1 << 20):
    return pl.pallas_call(
        kernel,
        out_shape=outs,
        in_specs=[space(pltpu.SMEM)] * len(smem)
        + [space(pltpu.HBM)] * len(hbm)
        + [space(pltpu.VMEM)] * len(vmem),
        out_specs=[space(kind) for kind in kinds],
        scratch_shapes=list(scratch),
        compiler_params=pltpu.CompilerParams(vmem_limit_bytes=limit * MIB),
        cost_estimate=pl.CostEstimate(flops=flops, transcendentals=0, bytes_accessed=1 << 20),
    )(*smem, *hbm, *vmem)


def quarter_shapes(width, sent):
    return [
        jax.ShapeDtypeStruct((128, width), jnp.float32 if k == 0 else sent) for k in range(4)
    ]


def over_rep(values):
    return {k: lax.ppermute(values[k], "zl", [(i, i ^ k) for i in range(4)]) for k in (1, 2, 3)}


def reduced(quarters, scale):
    total = quarters[0]
    for piece in over_rep(quarters).values():
        total = total + piece.astype(jnp.float32)
    scale = jnp.concatenate([scale] * (total.shape[1] // 128), axis=1)
    return (total / scale).astype(jnp.bfloat16)


def shared(value):
    got = over_rep([value] * 4)
    return [value, got[1], got[2], got[3]]


def per_device(
    features, tiles, tile_where, tile_count, degree, self_one, neigh_one, self_two, neigh_two
):
    early, late, groups, scale, weights = call(
        plan_kernel,
        (tile_where.reshape(SLOTS, 2).T, tile_count),
        (),
        (degree.reshape(4, 128), self_one, neigh_one),
        [
            jax.ShapeDtypeStruct((LISTED,), jnp.int32),
            jax.ShapeDtypeStruct((LISTED,), jnp.int32),
            jax.ShapeDtypeStruct((2,), jnp.int32),
            jax.ShapeDtypeStruct((128, 128), jnp.float32),
            jax.ShapeDtypeStruct((256, 256), jnp.bfloat16),
        ],
        [pltpu.SMEM] * 3 + [pltpu.VMEM] * 2,
        limit=2,
    )
    (tiles_held,) = call(
        load_kernel,
        (),
        (
            pltpu.with_memory_space_constraint(
                tiles.reshape(SLOTS, TILE, TILE), pltpu.HBM
            ),
        ),
        (),
        [pltpu.VMEM((SLOTS, TILE, TILE), jnp.bfloat16)],
        [pltpu.VMEM],
        [pltpu.SemaphoreType.DMA],
        2,
    )
    whole = pltpu.VMEM((NODES, 128), jnp.bfloat16)

    pieces = spread(features)
    *quarters, features_held = call(
        first_kernel,
        (early, late, groups),
        (),
        (tiles_held, *pieces),
        quarter_shapes(128, jnp.float32) + [whole],
        [pltpu.VMEM] * 5,
        [pltpu.VMEM((3 * TILE, 128), jnp.float32)],
        8,
        1 << 30,
    )

    agg_one = reduced(quarters, scale)
    (own_agg,) = call(
        arrange_kernel,
        (),
        (),
        shared(agg_one),
        [jax.ShapeDtypeStruct((512, 128), jnp.bfloat16)],
        [pltpu.VMEM],
    )
    own_hidden = jnp.dot(
        jnp.concatenate([features, own_agg], axis=1), weights, preferred_element_type=jnp.float32
    )
    own_hidden = jax.nn.relu(own_hidden).astype(jnp.bfloat16)
    own_part = jnp.dot(own_hidden, self_two, preferred_element_type=jnp.float32)

    pieces = spread(own_agg)
    (total,) = call(
        second_early,
        (early, groups),
        (),
        (tiles_held, features_held, weights, pieces[0], pieces[3]),
        [jax.ShapeDtypeStruct((3 * TILE, 256), jnp.float32)],
        [pltpu.VMEM],
        limit=4,
        flops=1 << 30,
    )
    quarters = call(
        second_late,
        (late, groups),
        (),
        (tiles_held, features_held, weights, total, *pieces[1:3], *pieces[4:]),
        quarter_shapes(256, jnp.bfloat16),
        [pltpu.VMEM] * 4,
        [whole, pltpu.VMEM((3 * TILE, 256), jnp.float32)],
        14,
        1 << 31,
    )

    (out,) = call(
        last_kernel,
        (),
        (),
        (own_part, neigh_two, *shared(reduced(quarters, scale))),
        [jax.ShapeDtypeStruct((512, 256), jnp.float32)],
        [pltpu.VMEM],
    )
    return out


def solution(mesh):
    wide = Mesh(mesh.devices.reshape(2, 4, 4, 2, 4), ("zh", "x", "y", "c", "zl"))
    return jax.shard_map(
        per_device,
        mesh=wide,
        in_specs=(
            P(ROW, None),
            P(ROW, "zl", None, None),
            P(ROW, "zl", None),
            P(ROW, "zl"),
            P(ROW),
            P(),
            P(),
            P(),
            P(),
        ),
        out_specs=P(ROW, None),
        check_vma=False,
    )
```

```python
import jax
import jax.numpy as jnp
from jax import lax
from jax.experimental import pallas as pl
from jax.experimental.pallas import tpu as pltpu
from jax.sharding import Mesh
from jax.sharding import PartitionSpec as P

TILE = 256
SLOTS = 64
UNROLL = 4
LISTED = SLOTS + UNROLL
NODES = 32768
MIB = 1 << 20


ROW = ("zh", "x", "y", "c")
PLANE = ("x", "y", "c")
ORDER = (1, 3, 2)
SWAP = [(0, 1), (1, 0)]


def in_plane(k, phase):
    pairs = []
    for x in range(4):
        for y in range(4):
            for c in range(2):
                along_x = (c + phase) % 2 == 0
                to_x, to_y = ((x + k) % 4, y) if along_x else (x, (y + k) % 4)
                pairs.append(((x * 4 + y) * 2 + c, (to_x * 4 + to_y) * 2 + c))
    return pairs


def hops(value, phase, order=ORDER):
    received = []
    for k in order:
        received.append(lax.ppermute(value, PLANE, in_plane(k, phase)))
    return received


def onward(one, three):
    half = one.shape[0] // 2
    top = lax.ppermute(one[:half], PLANE, in_plane(1, 1))
    bottom = lax.ppermute(three[half:], PLANE, in_plane(3, 1))
    return jnp.concatenate([top, bottom])


def spread(block):
    other = lax.ppermute(block, "zh", SWAP)
    own_line = jnp.concatenate([block, *hops(block, 0)])
    other_line = jnp.concatenate([other, *hops(other, 0)])
    one, three = hops(own_line, 1, (1, 3))
    own_near, own_two = jnp.concatenate([own_line, one, three]), onward(one, three)
    one, three = hops(other_line, 1, (1, 3))
    middle = jnp.concatenate([other_line, one, three, own_two])
    pieces = [own_near, middle, onward(one, three)]
    swapped = []
    for piece in pieces:
        swapped.append(lax.ppermute(piece, "c", SWAP))
    return pieces + swapped


def load_kernel(tiles, held, sem):
    load = pltpu.make_async_copy(tiles, held, sem)
    load.start()
    load.wait()


def plan_kernel(
    where, count, degree, self_one, neigh_one, first, second, late, groups, scale, weights
):
    my_zh, my_core = lax.axis_index("zh"), lax.axis_index("c")
    my_x, my_y = lax.axis_index("x"), lax.axis_index("y")

    def step(s, carry):
        n_first, n_second, n_late = carry
        segment, column = where[0, s], where[1, s]
        core = (column >> 1) & 1
        dy = (my_y - (column >> 2)) & 3
        dx = (my_x - (column >> 4)) & 3
        dy = dy ^ (dy >> 1)
        dx = dx ^ (dx >> 1)
        outer = jnp.where(core == 0, dy, dx)
        inner = jnp.where(core == 0, dx, dy)
        dz = (column >> 6) ^ my_zh
        part = jnp.where(outer == 3, 48 + dz * 8, dz * 24 + outer * 8)
        place = (core ^ my_core) * 64 + part + inner * 2 + (column & 1)
        code = s + segment * 256 + place * 65536
        first[n_first] = code
        second[n_second] = code
        late[n_late] = code
        is_late = jnp.where(outer == 3, 1, dz)
        swapped = (1 - is_late) * (core ^ my_core)
        return n_first + 1 - is_late - swapped, n_second + swapped, n_late + is_late

    counts = lax.fori_loop(0, count[0, 0], step, (0, 0, 0))
    for i, (listed, n) in enumerate(zip((first, second, late), counts)):
        for u in range(UNROLL):
            listed[n + u] = 2 * 256
        groups[i] = (n + UNROLL - 1) >> 2
    share = degree[pl.ds(lax.axis_index("zl"), 1), :].astype(jnp.float32)
    scale[...] = jnp.broadcast_to(share, (128, 128)).T
    weights[pl.ds(0, 128), :] = self_one[...]
    weights[pl.ds(128, 128), :] = neigh_one[...]


def gather_pieces(pieces, whole, base):
    for piece in pieces:

        def move(j, carry, base=base, piece=piece):
            source = pl.ds(pl.multiple_of(j * TILE, TILE), TILE)
            target = pl.ds(pl.multiple_of(base + j * TILE, TILE), TILE)
            whole[target, :] = piece[source, :]
            return carry

        lax.fori_loop(0, piece.shape[0] // TILE, move, 0)
        base += piece.shape[0]


def tile_rows(index):
    return pl.ds(pl.multiple_of(index * TILE, TILE), TILE)


def write_quarters(total, outs):
    me = lax.axis_index("zl")
    for k, out in enumerate(outs):
        start = pl.multiple_of((me ^ k) * 128, 128)
        out[...] = total[pl.ds(start, 128), :].astype(out.dtype)


def add_products(listed, groups, tiles, rows_of, total):
    def step(g, carry):
        codes = [listed[g * UNROLL + u] for u in range(UNROLL)]
        products = [
            jnp.dot(tiles[code & 255], rows_of(code >> 16), preferred_element_type=jnp.float32)
            for code in codes
        ]
        for code, product in zip(codes, products):
            total[tile_rows((code >> 8) & 255), :] += product
        return carry

    lax.fori_loop(0, groups, step, 0)


def hidden_rows(features, weights, agg):
    def rows_of(place):
        both = jnp.concatenate([features[tile_rows(place), :], agg(place)], axis=1)
        hidden = jnp.dot(both, weights[...], preferred_element_type=jnp.float32)
        return jnp.maximum(hidden, 0.0).astype(jnp.bfloat16)

    return rows_of


def first_kernel(first, second, late, groups, tiles, *refs):
    pieces, quarters, (whole, total) = refs[:6], refs[6:10], refs[10:]
    gather_pieces(pieces, whole, 0)
    total[...] = jnp.zeros_like(total)
    for which, listed in enumerate((first, second, late)):
        add_products(
            listed, groups[which], tiles, lambda place: whole[tile_rows(place), :], total
        )
    write_quarters(total, quarters)


def second_first(listed, groups, tiles, features, weights, piece, total):
    agg = lambda place: piece[tile_rows(place & 31), :]
    total[...] = jnp.zeros_like(total)
    add_products(listed, groups[0], tiles, hidden_rows(features, weights, agg), total)


def second_second(listed, groups, tiles, features, weights, before, piece, total):
    agg = lambda place: piece[tile_rows(place & 31), :]
    total[...] = before[...]
    add_products(listed, groups[1], tiles, hidden_rows(features, weights, agg), total)


def second_late(late, groups, tiles, features, weights, before, *refs):
    pieces, quarters, (whole, total) = refs[:4], refs[4:8], refs[8:]
    gather_pieces(pieces[:2], whole, 6144)
    gather_pieces(pieces[2:], whole, NODES // 2 + 6144)
    total[...] = before[...]
    agg = lambda place: whole[tile_rows(place), :]
    add_products(late, groups[2], tiles, hidden_rows(features, weights, agg), total)
    write_quarters(total, quarters)


def arrange_kernel(*refs):
    shares, out = refs[:4], refs[4]
    me = lax.axis_index("zl")
    for k, share in enumerate(shares):
        out[pl.ds(pl.multiple_of((me ^ k) * 128, 128), 128), :] = share[...]


def last_kernel(own, weights, *refs):
    shares, out = refs[:4], refs[4]
    me = lax.axis_index("zl")
    for k, share in enumerate(shares):
        rows = pl.ds(pl.multiple_of((me ^ k) * 128, 128), 128)
        out[rows, :] = own[rows, :] + jnp.dot(
            share[...], weights[...], preferred_element_type=jnp.float32
        )


def space(kind):
    return pl.BlockSpec(memory_space=kind)


def call(kernel, smem, hbm, vmem, outs, kinds, scratch=(), limit=4, flops=1 << 20):
    return pl.pallas_call(
        kernel,
        out_shape=outs,
        in_specs=[space(pltpu.SMEM)] * len(smem)
        + [space(pltpu.HBM)] * len(hbm)
        + [space(pltpu.VMEM)] * len(vmem),
        out_specs=[space(kind) for kind in kinds],
        scratch_shapes=list(scratch),
        compiler_params=pltpu.CompilerParams(vmem_limit_bytes=limit * MIB),
        cost_estimate=pl.CostEstimate(flops=flops, transcendentals=0, bytes_accessed=1 << 20),
    )(*smem, *hbm, *vmem)


def quarter_shapes(width, sent):
    return [
        jax.ShapeDtypeStruct((128, width), jnp.float32 if k == 0 else sent) for k in range(4)
    ]


def over_rep(values):
    return {k: lax.ppermute(values[k], "zl", [(i, i ^ k) for i in range(4)]) for k in (1, 2, 3)}


def reduced(quarters, scale):
    total = quarters[0]
    for piece in over_rep(quarters).values():
        total = total + piece.astype(jnp.float32)
    scale = jnp.concatenate([scale] * (total.shape[1] // 128), axis=1)
    return (total / scale).astype(jnp.bfloat16)


def shared(value):
    got = over_rep([value] * 4)
    return [value, got[1], got[2], got[3]]


def per_device(
    features, tiles, tile_where, tile_count, degree, self_one, neigh_one, self_two, neigh_two
):
    *lists, groups, scale, weights = call(
        plan_kernel,
        (tile_where.reshape(SLOTS, 2).T, tile_count),
        (),
        (degree.reshape(4, 128), self_one, neigh_one),
        [
            *[jax.ShapeDtypeStruct((LISTED,), jnp.int32)] * 3,
            jax.ShapeDtypeStruct((3,), jnp.int32),
            jax.ShapeDtypeStruct((128, 128), jnp.float32),
            jax.ShapeDtypeStruct((256, 256), jnp.bfloat16),
        ],
        [pltpu.SMEM] * 4 + [pltpu.VMEM] * 2,
        limit=2,
    )
    (tiles_held,) = call(
        load_kernel,
        (),
        (
            pltpu.with_memory_space_constraint(
                tiles.reshape(SLOTS, TILE, TILE), pltpu.HBM
            ),
        ),
        (),
        [pltpu.VMEM((SLOTS, TILE, TILE), jnp.bfloat16)],
        [pltpu.VMEM],
        [pltpu.SemaphoreType.DMA],
        2,
    )
    whole = pltpu.VMEM((NODES, 128), jnp.bfloat16)

    pieces = spread(features)
    *quarters, features_held = call(
        first_kernel,
        (*lists, groups),
        (),
        (tiles_held, *pieces),
        quarter_shapes(128, jnp.float32) + [whole],
        [pltpu.VMEM] * 5,
        [pltpu.VMEM((3 * TILE, 128), jnp.float32)],
        8,
        1 << 30,
    )

    agg_one = reduced(quarters, scale)
    (own_agg,) = call(
        arrange_kernel,
        (),
        (),
        shared(agg_one),
        [jax.ShapeDtypeStruct((512, 128), jnp.bfloat16)],
        [pltpu.VMEM],
    )
    own_hidden = jnp.dot(
        jnp.concatenate([features, own_agg], axis=1), weights, preferred_element_type=jnp.float32
    )
    own_hidden = jax.nn.relu(own_hidden).astype(jnp.bfloat16)
    own_part = jnp.dot(own_hidden, self_two, preferred_element_type=jnp.float32)

    pieces = spread(own_agg)
    part = [jax.ShapeDtypeStruct((3 * TILE, 256), jnp.float32)]
    (total,) = call(
        second_first,
        (lists[0], groups),
        (),
        (tiles_held, features_held, weights, pieces[0]),
        part,
        [pltpu.VMEM],
        limit=4,
        flops=1 << 29,
    )
    (total,) = call(
        second_second,
        (lists[1], groups),
        (),
        (tiles_held, features_held, weights, total, pieces[3]),
        part,
        [pltpu.VMEM],
        limit=4,
        flops=1 << 29,
    )
    quarters = call(
        second_late,
        (lists[2], groups),
        (),
        (tiles_held, features_held, weights, total, *pieces[1:3], *pieces[4:]),
        quarter_shapes(256, jnp.bfloat16),
        [pltpu.VMEM] * 4,
        [whole, pltpu.VMEM((3 * TILE, 256), jnp.float32)],
        14,
        1 << 31,
    )

    (out,) = call(
        last_kernel,
        (),
        (),
        (own_part, neigh_two, *shared(reduced(quarters, scale))),
        [jax.ShapeDtypeStruct((512, 256), jnp.float32)],
        [pltpu.VMEM],
    )
    return out


def solution(mesh):
    wide = Mesh(mesh.devices.reshape(2, 4, 4, 2, 4), ("zh", "x", "y", "c", "zl"))
    return jax.shard_map(
        per_device,
        mesh=wide,
        in_specs=(
            P(ROW, None),
            P(ROW, "zl", None, None),
            P(ROW, "zl", None),
            P(ROW, "zl"),
            P(ROW),
            P(),
            P(),
            P(),
            P(),
        ),
        out_specs=P(ROW, None),
        check_vma=False,
    )
```
